32 devices in a mesh: rep: 2 (over y), ep: 16 (over z, x, core).
Axes of the slice: x: 2, y: 2, z: 4, core: 2. Of those that a mesh axis runs over, the one named last changes fastest.
Arguments:
- cache_kv: bfloat16 [64, 2048, 576], P(('rep', 'ep')), parts along dimension 0, may hold values from -6 to 6
- new_kv: bfloat16 [64, 2, 576], P(('rep', 'ep')), parts along dimension 0, may hold values from -6 to 6
- queries: bfloat16 [64, 2, 64, 576], P(('rep', 'ep')), parts along dimension 0, may hold values from -256 to 256
- lengths: int32 [64], P(('rep', 'ep')), parts along dimension 0, may hold values from 256 to 2048
- resid: bfloat16 [64, 2, 7168], P(('rep', 'ep')), parts along dimension 0, may hold values from -18 to 18
- value_up: bfloat16 [512, 8192], P(None, 'ep'), may hold values from -1.5 to 1.5
- out_proj: bfloat16 [8192, 7168], P('ep'), may hold values from -0.09375 to 0.09375
- norm_gain: bfloat16 [7168], replicated, may hold values from 0.25 to 1.75
- router: bfloat16 [7168, 16], replicated, may hold values from -0.0625 to 0.0625
- expert_ids: int32 [64, 2, 8], P(('rep', 'ep')), parts along dimension 0, may hold values from 0 to 15, as said below
- slots: int32 [64, 2, 8], P(('rep', 'ep')), parts along dimension 0, may hold values from 0 to 3, as said below
- w_gate: bfloat16 [7168, 16384], P(None, 'ep'), may hold values from -0.0625 to 0.0625
- w_up: bfloat16 [7168, 16384], P(None, 'ep'), may hold values from -0.0625 to 0.0625
- w_down: bfloat16 [16384, 7168], P('ep'), may hold values from -0.1875 to 0.1875
Outputs:
- mixed: bfloat16 [64, 2, 7168], P(('rep', 'ep')), parts along dimension 0
The draws below stay inside these ranges and needn't reach their ends.
There are 2 independent parts, one for each index of `rep`. The reference program is written for one: setup_inputs(seed, part) draws one part's arguments, and reference() takes and returns one part's arrays. A program takes and returns all parts, laid end to end along the dimension named above; an argument that names none is the same for every part. Nothing has to cross between parts.
Inputs may be any that keep to these rules, and one draw needn't show every extreme that they name: `expert_ids`: each row names 8 different experts. In each aligned block of 4 rows (the rows of one device), the rows that name the same expert carry the distinct slots 0 up to their number minus one for it; in every block some expert is named by all 4 rows.
All inputs are finite; a program needn't handle non-finite values.
Results may differ from the reference program's by a relative error of at most 0.0065.
Values may be sent and summed in bfloat16 or wider, within the bound.
A program may use at most 128 MiB of HBM per device.

```python
import jax
import jax.numpy as jnp
from jax import lax

D = 7168
H = 64
LAT = 512
VH = 128
FFW = 1024
EXPERTS = 16
TOP = 8
CAP = 2
STEPS = 2
CACHE = 2048
KV = 576
QK = 192
TOK_DEV = 4
BATCH = 32
N_EP = 16


def attention_pair(key):
    cache_part = jax.random.truncated_normal(jax.random.fold_in(key, 21), -6.0, 6.0, (BATCH, CACHE, KV), jnp.float32)
    query_part = jax.random.truncated_normal(jax.random.fold_in(key, 22), -6.0, 6.0, (BATCH, STEPS, H, KV), jnp.float32)
    return (cache_part, query_part)


def draw_cache_kv(key, part):
    return attention_pair(key)[0].astype(jnp.bfloat16)


def draw_queries(key, part):
    return attention_pair(key)[1].astype(jnp.bfloat16)


def draw_resid(key, part):
    columns = jnp.exp(jax.random.uniform(jax.random.fold_in(key, 31), (D,), jnp.float32, jnp.log(0.3), jnp.log(3.0)))
    base = jax.random.truncated_normal(jax.random.fold_in(key, 34), -6.0, 6.0, (BATCH, STEPS, D), jnp.float32)
    return (base * columns).astype(jnp.bfloat16)


def routing_pair(key):
    rows_all = BATCH * STEPS
    blocks = rows_all // TOK_DEV
    expert_range = jnp.arange(EXPERTS, dtype=jnp.int32)
    base = jax.random.randint(jax.random.fold_in(key, 41), (rows_all, EXPERTS), 0, 1 << 20)
    order = jax.random.permutation(jax.random.fold_in(key, 42), EXPERTS).astype(jnp.int32)
    forced = jax.random.randint(jax.random.fold_in(key, 43), (blocks,), 0, EXPERTS)
    forced_rows = jnp.repeat(forced, TOK_DEV)
    boost = jnp.where(expert_range[None, :] == forced_rows[:, None], 1 << 24, 0)
    scores = (base + order[None, :] * (1 << 16) + boost) * EXPERTS + expert_range[None, :]
    _, chosen = lax.top_k(scores, TOP)
    chosen = chosen.astype(jnp.int32)
    row_in_block = jnp.arange(rows_all, dtype=jnp.int32) % TOK_DEV
    priority = jax.random.randint(jax.random.fold_in(key, 44), (rows_all, EXPERTS), 0, 1 << 20) * TOK_DEV + row_in_block[:, None]
    named = jnp.any(chosen[:, :, None] == expert_range[None, None, :], axis=1)
    named_block = named.reshape(blocks, TOK_DEV, EXPERTS)
    priority_block = priority.reshape(blocks, TOK_DEV, EXPERTS)
    earlier = named_block[:, None, :, :] & (priority_block[:, None, :, :] < priority_block[:, :, None, :])
    rank = jnp.sum(earlier.astype(jnp.int32), axis=2).reshape(rows_all, EXPERTS)
    slot_values = jnp.take_along_axis(rank, chosen, axis=1)
    return (chosen.reshape(BATCH, STEPS, TOP), slot_values.reshape(BATCH, STEPS, TOP))


def draw_expert_ids(key, part):
    return routing_pair(key)[0]


def draw_slots(key, part):
    return routing_pair(key)[1]


def set_ends(drawn, rng, least, high):
    longest = drawn.shape.index(max(drawn.shape))
    spots = []
    for shift in (0, 1):
        where = [jax.random.randint(jax.random.fold_in(rng, axis), (), 0, length) for axis, length in enumerate(drawn.shape)]
        where[longest] = (where[longest] + shift) % drawn.shape[longest]
        spots.append(tuple(where))
    return drawn.at[spots[0]].set(least).at[spots[1]].set(high)


def steps_of(rng, extent, cuts, smallest, top_value):
    factor_of, own = 1.0, jax.random.fold_in(rng, 6)
    for position, blocks in cuts:
        steps = jnp.exp(jax.random.uniform(jax.random.fold_in(own, position), (blocks,), jnp.float32, smallest / len(cuts), top_value / len(cuts)))
        factor_of = factor_of * jnp.repeat(steps, extent[position] // blocks).reshape([-1 if axis == position else 1 for axis in range(len(extent))])
    return factor_of


def normal_values(own_key, dims, deviation, bound, pieces=(), held_as=jnp.bfloat16):
    loudness = steps_of(own_key, dims, pieces, -0.22, 0.18) if pieces else 1.0
    values = jax.random.normal(own_key, dims, jnp.float32) * deviation * loudness
    return jnp.minimum(jnp.maximum(values, -bound), bound).astype(held_as)


def setup_inputs(seed: int = 0, part: int = 0) -> dict:
    key_list = jax.random.split(jax.random.key(seed), 15)
    part_splits = jax.random.split(jax.random.fold_in(key_list[14], part), 15)
    cache_kv = draw_cache_kv(jax.random.fold_in(jax.random.fold_in(key_list[14], part), 71), part)
    new_kv = normal_values(part_splits[1], (BATCH, STEPS, KV), 1.0, 6.0, ((0, 16),))
    queries = draw_queries(jax.random.fold_in(jax.random.fold_in(key_list[14], part), 71), part)
    lengths = set_ends(jax.random.randint(part_splits[3], (BATCH,), CACHE // 8, CACHE + 1), jax.random.fold_in(part_splits[3], 1), CACHE // 8, CACHE).astype(jnp.int32)
    resid = draw_resid(jax.random.fold_in(jax.random.fold_in(key_list[14], part), 71), part)
    value_up = normal_values(key_list[5], (LAT, H * VH), (max(1, LAT // 32)) ** -0.5, 1.5, ((1, 16),))
    out_proj = normal_values(key_list[6], (H * VH, D), (H * VH // 2) ** -0.5, 0.09375, ((0, 16),))
    norm_gain = jnp.clip(1.0 + 0.15 * jax.random.normal(key_list[7], (D,), jnp.float32), 0.25, 1.75).astype(jnp.bfloat16)
    router = normal_values(key_list[8], (D, EXPERTS), D ** -0.5, 0.0625)
    expert_ids = draw_expert_ids(jax.random.fold_in(jax.random.fold_in(key_list[14], part), 71), part)
    slots = draw_slots(jax.random.fold_in(jax.random.fold_in(key_list[14], part), 71), part)
    w_gate = normal_values(key_list[11], (D, EXPERTS * FFW), D ** -0.5, 0.0625, ((1, 16),))
    w_up = normal_values(key_list[12], (D, EXPERTS * FFW), D ** -0.5, 0.0625, ((1, 16),))
    w_down = normal_values(key_list[13], (EXPERTS * FFW, D), FFW ** -0.5, 0.1875, ((0, 16),))
    return dict(cache_kv=cache_kv, new_kv=new_kv, queries=queries, lengths=lengths, resid=resid, value_up=value_up, out_proj=out_proj, norm_gain=norm_gain, router=router, expert_ids=expert_ids, slots=slots, w_gate=w_gate, w_up=w_up, w_down=w_down)


route_scale = 2.827
norm_eps = 1e-06

def attend_one(packed):
    cache_rows, new_rows, query_rows, length = packed
    score_scale = 1.0 / QK ** 0.5
    query_full = query_rows.astype(jnp.float32)
    cache_full = cache_rows.astype(jnp.float32)
    new_full = new_rows.astype(jnp.float32)
    score_cache = jnp.einsum('shk,pk->shp', query_full, cache_full) * score_scale
    is_live = jnp.arange(CACHE, dtype=jnp.int32) < length
    score_cache = jnp.where(is_live[None, None, :], score_cache, -jnp.inf)
    score_new = jnp.einsum('shk,tk->sht', query_full, new_full) * score_scale
    step_ids = jnp.arange(STEPS, dtype=jnp.int32)
    causal = step_ids[None, :] <= step_ids[:, None]
    score_new = jnp.where(causal[:, None, :], score_new, -jnp.inf)
    row_peak = jnp.maximum(lax.optimization_barrier(jnp.max(score_cache, axis=-1)), lax.optimization_barrier(jnp.max(score_new, axis=-1)))
    exp_cache = jnp.exp(score_cache - row_peak[..., None])
    exp_new = jnp.exp(score_new - row_peak[..., None])
    exp_total = lax.optimization_barrier(jnp.sum(exp_cache, axis=-1)) + lax.optimization_barrier(jnp.sum(exp_new, axis=-1))
    prob_cache = (exp_cache / exp_total[..., None]).astype(jnp.bfloat16)
    prob_new = (exp_new / exp_total[..., None]).astype(jnp.bfloat16)
    context = jnp.einsum('shp,pc->shc', prob_cache.astype(jnp.float32), cache_full[:, :LAT])
    context = context + jnp.einsum('sht,tc->shc', prob_new.astype(jnp.float32), new_full[:, :LAT])
    return context.astype(jnp.bfloat16)

def reference(cache_kv, new_kv, queries, lengths, resid, value_up, out_proj, norm_gain, router, expert_ids, slots, w_gate, w_up, w_down):
    contexts = lax.map(attend_one, (cache_kv, new_kv, queries, lengths))
    values = jnp.einsum('bshc,chv->bshv', contexts.astype(jnp.float32), value_up.reshape(LAT, H, VH).astype(jnp.float32)).astype(jnp.bfloat16)
    rows_all = BATCH * STEPS
    attended = jnp.dot(values.reshape(rows_all, H * VH), out_proj, preferred_element_type=jnp.float32)
    hidden = resid.reshape(rows_all, D).astype(jnp.float32) + attended
    mean_square = lax.optimization_barrier(jnp.mean(hidden * hidden, axis=-1, keepdims=True))
    normed = (hidden * lax.rsqrt(mean_square + norm_eps) * norm_gain.astype(jnp.float32)).astype(jnp.bfloat16)
    logits = jnp.dot(normed, router, preferred_element_type=jnp.float32)
    route_ids = expert_ids.reshape(rows_all, TOP).astype(jnp.int32)
    route_slots = slots.reshape(rows_all, TOP).astype(jnp.int32)
    picked = jnp.take_along_axis(logits, route_ids, axis=1)
    gates = jax.nn.sigmoid(picked)
    weights = route_scale * gates / lax.optimization_barrier(jnp.sum(gates, axis=1, keepdims=True))
    is_kept = route_slots < CAP
    token_index = jnp.broadcast_to(jnp.arange(rows_all, dtype=jnp.int32)[:, None], (rows_all, TOP))
    source = token_index // TOK_DEV
    slot_total = EXPERTS * N_EP * CAP
    flat_slot = route_ids * (N_EP * CAP) + source * CAP + route_slots
    flat_slot = jnp.where(is_kept, flat_slot, slot_total).astype(jnp.int32)
    owner_row = jnp.full((slot_total + 1,), rows_all, dtype=jnp.int32).at[flat_slot.reshape(-1)].set(token_index.reshape(-1))
    share_row = jnp.zeros((slot_total + 1,), jnp.float32).at[flat_slot.reshape(-1)].set(weights.reshape(-1))
    owner_row = owner_row[:slot_total].reshape(EXPERTS, N_EP * CAP)
    share_row = share_row[:slot_total].reshape(EXPERTS, N_EP * CAP)
    padded = jnp.concatenate([normed, jnp.zeros((1, D), jnp.bfloat16)], axis=0)

    def expert_step(expert_mix, packed):
        expert_index, owners, shares = packed
        token_rows = padded[owners]
        gate_cols = lax.dynamic_slice_in_dim(w_gate, expert_index * FFW, FFW, 1)
        up_cols = lax.dynamic_slice_in_dim(w_up, expert_index * FFW, FFW, 1)
        down_rows = lax.dynamic_slice_in_dim(w_down, expert_index * FFW, FFW, 0)
        gate = jnp.dot(token_rows, gate_cols, preferred_element_type=jnp.float32)
        upward = jnp.dot(token_rows, up_cols, preferred_element_type=jnp.float32)
        act = (jax.nn.silu(gate) * upward).astype(jnp.bfloat16)
        produced = jnp.dot(act, down_rows, preferred_element_type=jnp.float32) * shares[:, None]
        return (expert_mix.at[owners].add(produced), None)
    start_mix = jnp.zeros((rows_all + 1, D), jnp.float32)
    expert_mix, _ = lax.scan(expert_step, start_mix, (jnp.arange(EXPERTS, dtype=jnp.int32), owner_row, share_row))
    mixed = (hidden + expert_mix[:rows_all]).astype(jnp.bfloat16)
    return mixed.reshape(BATCH, STEPS, D)
```

```python
import functools
import math

import jax
import jax.numpy as jnp
from jax import lax
from jax.experimental import pallas as pl
from jax.experimental.pallas import tpu as pltpu
from jax.sharding import PartitionSpec as P

H = 64
LAT = 512
VH = 128
EXPERTS = 16
TOP = 8
CAP = 2
QK = 192


route_scale = 2.827
norm_eps = 1e-06


F32 = jnp.float32
BF16 = jnp.bfloat16
CORES = 2
LINE = 4
CHUNKS = 7
LANES = 128
KEY_BLOCKS = 4

MERGED = (0, 1, 4, 7, 10, 12, 13)
SECOND = (0, 1, 4, 7)


def loop(count, step, start=0):
    lax.fori_loop(start, count, lambda i, carry: (step(i), carry)[1], 0)


def pipeline(stages, delays, extra=None):
    def step(t):
        for delay, stage in zip(delays, stages):
            pl.when((t >= delay) & (t < CHUNKS + delay))(functools.partial(stage, t - delay))
        if extra is not None:
            extra(t)

    loop(CHUNKS + delays[-1], step)


def layer_kernel(
    n,
    len_ref,
    new_hbm,
    gain_hbm,
    router_hbm,
    ids_hbm,
    slots_hbm,
    cache_hbm,
    query_hbm,
    resid_hbm,
    vu_hbm,
    op_hbm,
    wg_hbm,
    wu_hbm,
    wd_hbm,
    out_ref,
    vu,
    op,
    wg,
    wu,
    wd,
    keys,
    fresh,
    query,
    new_ref,
    gain_in,
    gain,
    router,
    ids_ref,
    slots_ref,
    resid,
    ctx32,
    ctx_ref,
    ctx_in,
    rows32,
    values,
    act,
    gate_acc,
    up_acc,
    hid,
    part,
    pair_sum,
    line_sum,
    in_core0,
    in_mid0,
    in_line0,
    in_core1,
    in_mid1,
    in_line1,
    block,
    gathered,
    share_out,
    share_in,
    share_all,
    w_sem,
    small_sem,
    key_sem,
    ctx_send,
    ctx_recv,
    share_sem,
    core_send,
    core_recv,
    mid_send,
    mid_recv,
    line_send,
    line_recv,
):
    me = lax.axis_index("ep")
    mids = n // (CORES * LINE)
    c = me % CORES
    b = (me // CORES) % mids
    a = me // (CORES * mids)
    seqs, steps, width = resid.shape
    toks = seqs * steps
    part_w = width // CHUNKS
    piece = ctx_ref.shape[2]
    heads_per = piece // steps
    value_cols = vu.shape[1]
    total = n * toks
    fan = CORES * mids
    group = LINE * toks

    def dev(aa, bb, cc):
        return (aa * mids + bb) * CORES + cc

    def slot(aa, bb, cc):
        return (cc * mids + bb) * LINE + aa

    my_slot = slot(a, b, c)
    far_first = (LINE - 1 - a, (a + 2) % LINE, a + 1 - 2 * (a % 2))

    def send(src, dst, s_sem, r_sem, target):
        return pltpu.make_async_remote_copy(
            src_ref=src,
            dst_ref=dst,
            send_sem=s_sem,
            recv_sem=r_sem,
            device_id={"ep": target},
            device_id_type=pl.DeviceIdType.MESH,
        )

    def settle(ref, sem):
        pltpu.make_async_copy(ref, ref, sem).wait()

    def cols(ch):
        return pl.ds(pl.multiple_of(ch * part_w, part_w), part_w)

    def op_copy(ch):
        return pltpu.make_async_copy(op_hbm.at[:, cols(ch)], op.at[ch], w_sem.at[0, ch])

    def wg_copy(ch):
        return pltpu.make_async_copy(wg_hbm.at[cols(ch), :], wg.at[ch], w_sem.at[1, ch])

    def wu_copy(ch):
        return pltpu.make_async_copy(wu_hbm.at[cols(ch), :], wu.at[ch], w_sem.at[2, ch])

    def wd_copy(ch):
        return pltpu.make_async_copy(wd_hbm.at[:, cols(ch)], wd.at[ch], w_sem.at[3, ch])

    cache_len = cache_hbm.shape[2]
    key_w = cache_len // KEY_BLOCKS

    def key_copy(q, j):
        span = pl.ds(j * key_w, key_w)
        return pltpu.make_async_copy(
            cache_hbm.at[q, :, span], keys.at[q, :, span], key_sem.at[q, j]
        )

    def query_copy(q):
        return pltpu.make_async_copy(query_hbm.at[q], query.at[q], key_sem.at[q, KEY_BLOCKS])

    new_copy = pltpu.make_async_copy(new_hbm, new_ref, small_sem.at[0])
    vu_copy = pltpu.make_async_copy(vu_hbm, vu, small_sem.at[1])
    resid_copy = pltpu.make_async_copy(resid_hbm, resid, small_sem.at[2])
    gain_copy = pltpu.make_async_copy(gain_hbm, gain_in, small_sem.at[3])
    router_copy = pltpu.make_async_copy(router_hbm, router, small_sem.at[4])
    ids_copy = pltpu.make_async_copy(ids_hbm, ids_ref, small_sem.at[5])
    slots_copy = pltpu.make_async_copy(slots_hbm, slots_ref, small_sem.at[6])

    new_copy.start()
    for q in range(seqs):
        query_copy(q).start()
        for j in range(KEY_BLOCKS):
            key_copy(q, j).start()
    for small in (vu_copy, resid_copy, gain_copy, router_copy, ids_copy, slots_copy):
        small.start()

    barrier = pltpu.get_barrier_semaphore()

    def greet(i):
        pl.semaphore_signal(
            barrier,
            inc=1,
            device_id={"ep": (me + i) % n},
            device_id_type=pl.DeviceIdType.MESH,
        )

    loop(n, greet, 1)
    loop(CHUNKS, lambda ch: op_copy(ch).start())

    def start_ffn(ch):
        wg_copy(ch).start()
        wu_copy(ch).start()

    loop(CHUNKS, start_ffn)
    loop(CHUNKS, lambda ch: wd_copy(ch).start())

    rows_q, span_new = query.shape[1], fresh.shape[1]
    heads = rows_q // steps
    score_scale = math.log2(math.e) / math.sqrt(QK)
    fresh[...] = jnp.zeros_like(fresh)
    gate_acc[...] = jnp.zeros_like(gate_acc)
    up_acc[...] = jnp.zeros_like(up_acc)
    share_out[...] = jnp.zeros_like(share_out)
    newer = lax.broadcasted_iota(jnp.int32, (rows_q, span_new), 1) <= (
        lax.broadcasted_iota(jnp.int32, (rows_q, span_new), 0) // heads
    )
    place = lax.broadcasted_iota(jnp.int32, (rows_q, key_w), 1)
    across = (((1,), (1,)), ((), ()))

    def attend(q):
        query_copy(q).wait()
        new = lax.dot_general(query[q], fresh[q], across, preferred_element_type=F32)
        new = jnp.where(newer, new, -jnp.inf)
        peak = jnp.max(new, axis=-1, keepdims=True)
        for j in range(KEY_BLOCKS):
            key_copy(q, j).wait()
        old = []
        for j in range(KEY_BLOCKS):
            score = jnp.dot(
                query[q], keys[q, :, j * key_w : (j + 1) * key_w], preferred_element_type=F32
            )
            score = jnp.where(place < len_ref[q] - j * key_w, score, -jnp.inf)
            peak = jnp.maximum(peak, jnp.max(score, axis=-1, keepdims=True))
            old.append(score)
        new = jnp.exp2((new - peak) * score_scale)
        weight = jnp.sum(new, axis=-1, keepdims=True)
        context = jnp.dot(new.astype(BF16), fresh[q, :, :LAT], preferred_element_type=F32)
        for j in range(KEY_BLOCKS):
            prob = jnp.exp2((old[j] - peak) * score_scale)
            weight = weight + jnp.sum(prob, axis=-1, keepdims=True)
            context = context + lax.dot_general(
                prob.astype(BF16),
                keys[q, :LAT, j * key_w : (j + 1) * key_w],
                across,
                preferred_element_type=F32,
            )
        ctx32[q] = context * (1.0 / weight)
        for j in range(n):
            first = (j * value_cols) // VH
            rows = [
                ctx32[q, t * heads + first : t * heads + first + heads_per, :]
                for t in range(steps)
            ]
            ctx_ref[q, j] = jnp.concatenate(rows, axis=0).astype(BF16)

    def ctx_start(q):
        def one(to):
            send(
                ctx_ref.at[q, to],
                ctx_in.at[q, my_slot],
                ctx_send.at[0],
                ctx_recv.at[q],
                to,
            ).start()

        for aa in far_first:
            loop(fan, lambda i: one(aa * fan + (me + i) % fan))
        loop(fan, lambda i: one(a * fan + (me + i) % fan), 1)

    new_copy.wait()
    for q in range(seqs):
        fresh[q, :steps, :] = new_ref[q]
    with jax.named_scope("attn0"):
        attend(0)
    with jax.named_scope("barrier"):
        pl.semaphore_wait(barrier, n - 1)
    with jax.named_scope("send0"):
        ctx_start(0)
    for q in range(1, seqs):
        with jax.named_scope("attn1"):
            attend(q)
        with jax.named_scope("send1"):
            ctx_start(q)

    with jax.named_scope("prep"):
        ids_copy.wait()
        slots_copy.wait()
        lane = lax.broadcasted_iota(jnp.int32, (toks, EXPERTS), 1)
        named = jnp.zeros((toks, EXPERTS), F32)
        kept = jnp.zeros((toks, EXPERTS), F32)
        for k in range(TOP):
            hit = jnp.where(ids_ref[:, k : k + 1] == lane, 1.0, 0.0)
            named = named + hit
            kept = kept + jnp.where(slots_ref[:, k : k + 1] < CAP, hit, 0.0)
        resid_copy.wait()
        gain_copy.wait()
        per = part_w // LANES
        for ch in range(CHUNKS):
            rows = [resid[q, :, ch * part_w : (ch + 1) * part_w].astype(F32) for q in range(seqs)]
            hid[ch] = jnp.concatenate(rows, axis=0)
            wide = gain_in[ch * per : (ch + 1) * per, :].astype(F32)
            gain[ch] = jnp.concatenate([wide[k : k + 1] for k in range(per)], axis=1)
        vu_copy.wait()

    def fold_values(q):
        settle(ctx_in.at[q, pl.ds(0, n - 1)], ctx_recv.at[q])
        bunch = 8 // piece

        def put(g):
            tile = [ctx_in[q, g * bunch + h].astype(F32) for h in range(bunch)]
            rows32[pl.ds(pl.multiple_of(g * 8, 8), 8), :] = (
                jnp.concatenate(tile, axis=0) if bunch > 1 else tile[0]
            )

        loop(n // bunch, put)
        mixed = jnp.dot(rows32[...].astype(BF16), vu[...], preferred_element_type=F32)
        shape = (n * piece, value_cols)
        row_head = lax.broadcasted_iota(jnp.int32, shape, 0) % heads_per
        col_head = lax.broadcasted_iota(jnp.int32, shape, 1) // (value_cols // heads_per)
        mixed = jnp.where(row_head == col_head, mixed, 0.0).astype(BF16)
        shape = (total, n * piece)
        came = lax.broadcasted_iota(jnp.int32, shape, 1)
        row_tok = (came // piece) * toks + q * steps + (came % piece) // heads_per
        fold = jnp.where(row_tok == lax.broadcasted_iota(jnp.int32, shape, 0), 1.0, 0.0)
        return jnp.dot(fold.astype(BF16), mixed, preferred_element_type=F32)

    for q in range(seqs):
        ctx_in[q, my_slot] = ctx_ref[q, me]
    folded = None
    for q in range(seqs):
        with jax.named_scope("values"):
            term = fold_values(q)
            folded = term if folded is None else folded + term
    values[...] = folded.astype(BF16)

    def reduce_scatter(which, product, finish):
        in_core, in_mid, in_line = (
            (in_core0, in_mid0, in_line0) if which == 0 else (in_core1, in_mid1, in_line1)
        )

        def core_copy(ch):
            return send(
                part.at[ch, 1 - c],
                in_core.at[ch],
                core_send.at[which],
                core_recv.at[which, ch],
                dev(a, b, 1 - c),
            )

        def mid_copy(ch, bb):
            return send(
                pair_sum.at[ch, bb],
                in_mid.at[ch, b],
                mid_send.at[which],
                mid_recv.at[which, ch],
                dev(a, bb, c),
            )

        def line_copy(ch, aa):
            return send(
                line_sum.at[ch, aa],
                in_line.at[ch, a],
                line_send.at[which],
                line_recv.at[which, ch],
                dev(aa, b, c),
            )

        def stage1(ch):
            whole = product(ch).astype(BF16).reshape(CORES, mids, group, part_w)
            part[ch] = whole
            core_copy(ch).start()

        def stage2(ch):
            settle(in_core.at[ch], core_recv.at[which, ch])

            def pair(bb):
                pair_sum[ch, bb] = (
                    part[ch, c, bb].astype(F32) + in_core[ch, bb].astype(F32)
                ).astype(BF16)

            def pair_send(i):
                bb = (b + i) % mids
                pair(bb)
                mid_copy(ch, bb).start()

            loop(mids, pair_send, 1)
            pair(b)

        def stage3(ch):
            settle(in_mid.at[ch, pl.ds(0, mids - 1)], mid_recv.at[which, ch])
            acc = pair_sum[ch, b].astype(F32)
            acc = lax.fori_loop(
                1, mids, lambda i, t: t + in_mid[ch, (b + i) % mids].astype(F32), acc
            )
            for aa in range(LINE):
                line_sum[ch, aa] = acc[aa * toks : (aa + 1) * toks].astype(BF16)
            for aa in far_first:
                line_copy(ch, aa).start()

        def stage4(ch):
            settle(in_line.at[ch, pl.ds(0, LINE - 1)], line_recv.at[which, ch])
            acc = line_sum[ch, a].astype(F32)
            for aa in far_first:
                acc = acc + in_line[ch, aa].astype(F32)
            finish(ch, acc)

        def drain():
            settle(in_core, core_send.at[which])
            settle(in_mid.at[:, pl.ds(0, mids - 1)], mid_send.at[which])
            settle(in_line.at[:, pl.ds(0, LINE - 1)], line_send.at[which])

        return (stage1, stage2, stage3, stage4), drain

    def attended_part(ch):
        op_copy(ch).wait()
        return jnp.dot(values[...], op[ch], preferred_element_type=F32)

    def spread_hidden(ch, acc):
        hidden = hid[ch] + acc
        hid[ch] = hidden
        block[ch, a] = (hidden * gain[ch]).astype(BF16)
        for aa in far_first:
            send(
                block.at[ch, a],
                block.at[ch, a],
                line_send.at[2],
                line_recv.at[2, ch],
                dev(aa, b, c),
            ).start()

    def hop_mid(ch):
        settle(block.at[ch, pl.ds(0, LINE - 1)], line_recv.at[2, ch])
        rows = [block[ch, aa].astype(F32) for aa in range(LINE)]
        gathered[ch, c, b] = jnp.concatenate(rows, axis=0).astype(BF16)
        ours = gathered.at[ch, c, b]

        def forward(i):
            send(
                ours, ours, mid_send.at[2], mid_recv.at[2, ch], dev(a, (b + i) % mids, c)
            ).start()

        loop(mids, forward, 1)

    def hop_core(ch):
        settle(gathered.at[ch, c, pl.ds(0, mids - 1)], mid_recv.at[2, ch])
        ours = gathered.at[ch, c]
        send(ours, ours, core_send.at[2], core_recv.at[2, ch], dev(a, b, 1 - c)).start()

    def multiply(ch):
        settle(gathered.at[ch, 1 - c], core_recv.at[2, ch])
        rows = gathered[ch].reshape(total, part_w)
        wg_copy(ch).wait()
        gate_acc[...] += jnp.dot(rows, wg[ch], preferred_element_type=F32)
        wu_copy(ch).wait()
        up_acc[...] += jnp.dot(rows, wu[ch], preferred_element_type=F32)

    def route():
        router_copy.wait()
        square = jnp.zeros((toks, part_w), F32)
        logits = jnp.zeros((toks, EXPERTS), F32)
        for ch in range(CHUNKS):
            hidden = hid[ch]
            square = square + hidden * hidden
            logits = logits + lax.dot_general(
                block[ch, a],
                router[:, ch * part_w : (ch + 1) * part_w],
                across,
                preferred_element_type=F32,
            )
        scale = lax.rsqrt(jnp.sum(square, axis=-1, keepdims=True) / width + norm_eps)
        gates = jax.nn.sigmoid(logits * scale)
        shares = route_scale * gates / jnp.sum(gates * named, axis=1, keepdims=True) * kept
        share_out[:, :EXPERTS] = shares
        share_out[:, EXPERTS : EXPERTS + 1] = scale

        def share_start(i):
            send(
                share_out, share_in.at[my_slot], share_sem.at[0], share_sem.at[1], (me + i) % n
            ).start()

        loop(n, share_start, 1)
        share_in[my_slot] = share_out[...]

    first_stages, first_drain = reduce_scatter(0, attended_part, spread_hidden)

    def scoped(f):
        def g(*args):
            with jax.named_scope(f.__name__):
                f(*args)

        return g

    with jax.named_scope("merged"):
        pipeline(
            [scoped(f) for f in first_stages + (hop_mid, hop_core, multiply)],
            MERGED,
            lambda t: pl.when(t == CHUNKS + MERGED[3] - 1)(scoped(route)),
        )

    with jax.named_scope("act"):
        settle(share_in.at[pl.ds(0, n - 1)], share_sem.at[1])
        bunch = 8 // toks

        def put_share(g):
            tile = [share_in[g * bunch + h] for h in range(bunch)]
            share_all[pl.ds(pl.multiple_of(g * 8, 8), 8), :] = (
                jnp.concatenate(tile, axis=0) if bunch > 1 else tile[0]
            )

        loop(n // bunch, put_share)
        sent = share_all[...]
        mine = lax.broadcasted_iota(jnp.int32, share_all.shape, 1) == me // (n // EXPERTS)
        share = jnp.sum(jnp.where(mine, sent, 0.0), axis=1, keepdims=True)
        scale = sent[:, EXPERTS : EXPERTS + 1]
        gate = gate_acc[...] * scale
        act[...] = (gate * jax.nn.sigmoid(gate) * up_acc[...] * (scale * share)).astype(BF16)
        first_drain()

    def expert_part(ch):
        wd_copy(ch).wait()
        return jnp.dot(act[...], wd[ch], preferred_element_type=F32)

    def put_out(ch, acc):
        mixed = hid[ch] + acc
        for q in range(seqs):
            out_ref[q, :, cols(ch)] = mixed[q * steps : (q + 1) * steps].astype(BF16)

    second_stages, second_drain = reduce_scatter(1, expert_part, put_out)
    with jax.named_scope("rs2"):
        pipeline([scoped(f) for f in second_stages], SECOND)

    with jax.named_scope("drain"):
        second_drain()
        settle(ctx_in.at[:, pl.ds(0, n - 1)], ctx_send.at[0])
        settle(share_in.at[pl.ds(0, n - 1)], share_sem.at[0])
        settle(block.at[:, pl.ds(0, LINE - 1)], line_send.at[2])
        settle(gathered.at[:, 0, pl.ds(0, mids - 1)], mid_send.at[2])
        settle(gathered.at[:, 0], core_send.at[2])


def body(
    cache_kv,
    new_kv,
    queries,
    lengths,
    resid,
    value_up,
    out_proj,
    norm_gain,
    router,
    expert_ids,
    slots,
    w_gate,
    w_up,
    w_down,
):
    n = lax.axis_size("ep")
    seqs, steps, heads, kv = queries.shape
    toks = seqs * steps
    width = resid.shape[-1]
    heads_per = max(1, value_up.shape[1] // VH)
    packets = (seqs, n, steps * heads_per, LAT)
    hidden_units = w_gate.shape[1]
    mids = n // (CORES * LINE)
    part_w = width // CHUNKS
    total = n * toks
    group = LINE * toks
    vmem = pl.BlockSpec(memory_space=pltpu.VMEM)
    hbm = pl.BlockSpec(memory_space=pl.ANY)
    landing = [
        pltpu.VMEM((CHUNKS, mids, group, part_w), BF16),
        pltpu.VMEM((CHUNKS, mids, group, part_w), BF16),
        pltpu.VMEM((CHUNKS, LINE, toks, part_w), BF16),
    ]
    dma = pltpu.SemaphoreType.DMA
    mixed = pl.pallas_call(
        functools.partial(layer_kernel, n),
        out_shape=jax.ShapeDtypeStruct(resid.shape, BF16),
        in_specs=[pl.BlockSpec(memory_space=pltpu.SMEM)] + [hbm] * 13,
        out_specs=vmem,
        scratch_shapes=[
            pltpu.VMEM(value_up.shape, BF16),
            pltpu.VMEM((CHUNKS, out_proj.shape[0], part_w), BF16),
            pltpu.VMEM((CHUNKS, part_w, hidden_units), BF16),
            pltpu.VMEM((CHUNKS, part_w, hidden_units), BF16),
            pltpu.VMEM((CHUNKS, hidden_units, part_w), BF16),
            pltpu.VMEM((seqs, kv, cache_kv.shape[1]), BF16),
            pltpu.VMEM((seqs, LANES, kv), BF16),
            pltpu.VMEM((seqs, steps * heads, kv), BF16),
            pltpu.VMEM(new_kv.shape, BF16),
            pltpu.VMEM((width // LANES, LANES), BF16),
            pltpu.VMEM((CHUNKS, 1, part_w), F32),
            pltpu.VMEM((router.shape[1], width), BF16),
            pltpu.VMEM((toks, TOP), jnp.int32),
            pltpu.VMEM((toks, TOP), jnp.int32),
            pltpu.VMEM(resid.shape, BF16),
            pltpu.VMEM((seqs, steps * heads, LAT), F32),
            pltpu.VMEM(packets, BF16),
            pltpu.VMEM(packets, BF16),
            pltpu.VMEM((n * steps * heads_per, LAT), F32),
            pltpu.VMEM((total, value_up.shape[1]), BF16),
            pltpu.VMEM((total, hidden_units), BF16),
            pltpu.VMEM((total, hidden_units), F32),
            pltpu.VMEM((total, hidden_units), F32),
            pltpu.VMEM((CHUNKS, toks, part_w), F32),
            pltpu.VMEM((CHUNKS, CORES, mids, group, part_w), BF16),
            pltpu.VMEM((CHUNKS, mids, group, part_w), BF16),
            pltpu.VMEM((CHUNKS, LINE, toks, part_w), BF16),
            *landing,
            *landing,
            pltpu.VMEM((CHUNKS, LINE, toks, part_w), BF16),
            pltpu.VMEM((CHUNKS, CORES, mids, group, part_w), BF16),
            pltpu.VMEM((toks, LANES), F32),
            pltpu.VMEM((n, toks, LANES), F32),
            pltpu.VMEM((total, LANES), F32),
            dma((4, CHUNKS)),
            dma((7,)),
            dma((seqs, KEY_BLOCKS + 1)),
            dma((1,)),
            dma((seqs,)),
            dma((2,)),
            dma((3,)),
            dma((3, CHUNKS)),
            dma((3,)),
            dma((3, CHUNKS)),
            dma((3,)),
            dma((3, CHUNKS)),
        ],
        compiler_params=pltpu.CompilerParams(
            collective_id=0, has_side_effects=True, vmem_limit_bytes=67043328
        ),
    )(
        lengths,
        new_kv,
        norm_gain.reshape(width // LANES, LANES),
        router.T,
        expert_ids.reshape(toks, TOP),
        slots.reshape(toks, TOP),
        cache_kv.transpose(0, 2, 1),
        queries.reshape(seqs, steps * heads, kv),
        resid,
        value_up,
        out_proj,
        w_gate,
        w_up,
        w_down,
    )
    return mixed


def solution(mesh):
    return jax.shard_map(
        body,
        mesh=mesh,
        in_specs=(
            P(("rep", "ep"), None, None),
            P(("rep", "ep"), None, None),
            P(("rep", "ep"), None, None, None),
            P(("rep", "ep")),
            P(("rep", "ep"), None, None),
            P(None, "ep"),
            P("ep", None),
            P(),
            P(),
            P(("rep", "ep"), None, None),
            P(("rep", "ep"), None, None),
            P(None, "ep"),
            P(None, "ep"),
            P("ep", None),
        ),
        out_specs=P(("rep", "ep"), None, None),
        check_vma=False,
    )
```

```python
import functools
import math

import jax
import jax.numpy as jnp
from jax import lax
from jax.experimental import pallas as pl
from jax.experimental.pallas import tpu as pltpu
from jax.sharding import PartitionSpec as P

H = 64
LAT = 512
VH = 128
EXPERTS = 16
TOP = 8
CAP = 2
QK = 192


route_scale = 2.827
norm_eps = 1e-06


F32 = jnp.float32
BF16 = jnp.bfloat16
CORES = 2
LINE = 4
CHUNKS = 7
LANES = 128
WEIGHT_CUTS = 4
KEY_BLOCKS = 2

LATENCY = {"core": 1.0, "mid": 2.3, "line": 3.0}
OCCUPY = {"core": 0.7, "mid": 4.9, "line": 4.9}


def loop(count, step, start=0):
    lax.fori_loop(start, count, lambda i, carry: (step(i), carry)[1], 0)


def plan(work, hops):
    last = len(work) - 1
    ready = {(0, ch): 0.0 for ch in range(CHUNKS)}
    upcoming = [0] * len(work)
    free = dict.fromkeys(LATENCY, 0.0)
    now, order = 0.0, []
    while len(order) < CHUNKS * len(work):
        open_events = [
            (ready[stage, ch], stage, ch)
            for stage, ch in enumerate(upcoming)
            if (stage, ch) in ready
        ]
        runnable = [event for event in open_events if event[0] <= now + 1e-9]
        if runnable:
            late = (0, last) if last > 3 else (0,)
            _, stage, ch = min(runnable, key=lambda e: (e[1] in late[1:], e[1] in late, -e[1]))
        else:
            now, stage, ch = min(open_events)
        now += work[stage]
        order.append((stage, ch))
        upcoming[stage] += 1
        if stage < last:
            hop = hops[stage]
            free[hop] = max(free[hop], now) + OCCUPY[hop] / CHUNKS
            ready[stage + 1, ch] = free[hop] + LATENCY[hop]
    return order


def share_of(times):
    return [0.05 + time / CHUNKS for time in times]


MERGED = plan(
    share_of((2.0, 0.35, 0.35, 0.5, 0.35, 0.0, 5.7)),
    ("core", "mid", "line", "line", "mid", "core"),
)
SECOND = plan(share_of((3.1, 0.35, 0.35, 0.5)), ("core", "mid", "line"))


def layer_kernel(
    n,
    len_ref,
    new_hbm,
    gain_hbm,
    router_hbm,
    ids_hbm,
    slots_hbm,
    cache_hbm,
    query_hbm,
    resid_hbm,
    vu_hbm,
    op_hbm,
    wg_hbm,
    wu_hbm,
    wd_hbm,
    out_hbm,
    vu,
    op,
    wgu,
    wd,
    keys,
    fresh,
    query,
    new_ref,
    gain_in,
    gain,
    router,
    ids_ref,
    slots_ref,
    resid,
    ctx32,
    ctx_ref,
    ctx_in,
    rows32,
    values,
    act,
    ffn_acc,
    hid,
    part,
    pair_sum,
    line_sum,
    in_core,
    in_mid,
    in_line,
    block,
    gathered,
    share_out,
    share_in,
    share_all,
    out_ref,
    out_sem,
    w_sem,
    small_sem,
    key_sem,
    ctx_send,
    ctx_recv,
    share_sem,
    core_send,
    core_recv,
    mid_send,
    mid_recv,
    line_send,
    line_recv,
):
    me = lax.axis_index("ep")
    mids = n // (CORES * LINE)
    c = me % CORES
    b = (me // CORES) % mids
    a = me // (CORES * mids)
    seqs, steps, width = resid.shape
    toks = seqs * steps
    part_w = width // CHUNKS
    piece = ctx_ref.shape[2]
    heads_per = piece // steps
    value_cols = vu.shape[1]
    hidden_units = wd.shape[0]
    total = n * toks
    fan = CORES * mids
    group = LINE * toks

    def dev(aa, bb, cc):
        return (aa * mids + bb) * CORES + cc

    def slot(aa, bb, cc):
        return (cc * mids + bb) * LINE + aa

    my_slot = slot(a, b, c)
    far_first = (LINE - 1 - a, (a + 2) % LINE, a + 1 - 2 * (a % 2))

    def send(src, dst, s_sem, r_sem, target):
        return pltpu.make_async_remote_copy(
            src_ref=src,
            dst_ref=dst,
            send_sem=s_sem,
            recv_sem=r_sem,
            device_id={"ep": target},
            device_id_type=pl.DeviceIdType.MESH,
        )

    def settle(ref, sem):
        pltpu.make_async_copy(ref, ref, sem).wait()

    def cols(ch):
        return pl.ds(ch * part_w, part_w)

    def weight_start(hbm, vmem, sem):
        tall = hbm.shape[0] // WEIGHT_CUTS

        def one(k):
            span = pl.ds(pl.multiple_of(k * tall, tall), tall)
            pltpu.make_async_copy(hbm.at[span], vmem.at[span], sem).start()

        loop(WEIGHT_CUTS, one)

    w_gate = wgu.at[:, pl.ds(0, hidden_units)]
    w_up = wgu.at[:, pl.ds(hidden_units, hidden_units)]

    cache_len = cache_hbm.shape[2]
    key_w = cache_len // KEY_BLOCKS

    def key_copy(q, j):
        span = pl.ds(j * key_w, key_w)
        return pltpu.make_async_copy(
            cache_hbm.at[q, :, span], keys.at[q, :, span], key_sem.at[q, j]
        )

    def query_copy(q):
        return pltpu.make_async_copy(query_hbm.at[q], query.at[q], key_sem.at[q, KEY_BLOCKS])

    new_copy = pltpu.make_async_copy(new_hbm, new_ref, small_sem.at[0])
    vu_copy = pltpu.make_async_copy(vu_hbm, vu, small_sem.at[1])
    resid_copy = pltpu.make_async_copy(resid_hbm, resid, small_sem.at[2])
    gain_copy = pltpu.make_async_copy(gain_hbm, gain_in, small_sem.at[3])
    router_copy = pltpu.make_async_copy(router_hbm, router, small_sem.at[4])
    ids_copy = pltpu.make_async_copy(ids_hbm, ids_ref, small_sem.at[5])
    slots_copy = pltpu.make_async_copy(slots_hbm, slots_ref, small_sem.at[6])

    def keys_start(q):
        query_copy(q).start()
        for j in range(KEY_BLOCKS):
            key_copy(q, j).start()

    keys_start(0)
    new_copy.start()

    barrier = pltpu.get_barrier_semaphore()

    def greet(i):
        pl.semaphore_signal(
            barrier,
            inc=1,
            device_id={"ep": (me + i) % n},
            device_id_type=pl.DeviceIdType.MESH,
        )

    loop(n, greet, 1)

    for q in range(1, seqs):
        keys_start(q)
    for small in (vu_copy, resid_copy, gain_copy, router_copy, ids_copy, slots_copy):
        small.start()

    def start_weights():
        weight_start(op_hbm, op, w_sem.at[0])
        weight_start(wg_hbm, w_gate, w_sem.at[1])
        weight_start(wu_hbm, w_up, w_sem.at[2])
        weight_start(wd_hbm, wd, w_sem.at[3])

    rows_q, span_new = query.shape[1], fresh.shape[1]
    heads = rows_q // steps
    score_scale = math.log2(math.e) / math.sqrt(QK)
    fresh[...] = jnp.zeros_like(fresh)
    newer = lax.broadcasted_iota(jnp.int32, (rows_q, span_new), 1) <= (
        lax.broadcasted_iota(jnp.int32, (rows_q, span_new), 0) // heads
    )
    place = lax.broadcasted_iota(jnp.int32, (rows_q, key_w), 1)
    across = (((1,), (1,)), ((), ()))

    def attend(q):
        def keys_here():
            for j in range(KEY_BLOCKS):
                key_copy(q, j).wait()
            if q == seqs - 1:
                start_weights()

        query_copy(q).wait()
        if q > 0:
            keys_here()
        new = lax.dot_general(query[q], fresh[q], across, preferred_element_type=F32)
        new = jnp.where(newer, new, -jnp.inf)
        peak = jnp.max(new, axis=-1, keepdims=True)
        if q == 0:
            keys_here()
        old = []
        for j in range(KEY_BLOCKS):
            score = jnp.dot(
                query[q], keys[q, :, j * key_w : (j + 1) * key_w], preferred_element_type=F32
            )
            score = jnp.where(place < len_ref[q] - j * key_w, score, -jnp.inf)
            peak = jnp.maximum(peak, jnp.max(score, axis=-1, keepdims=True))
            old.append(score)
        new = jnp.exp2((new - peak) * score_scale)
        weight = jnp.sum(new, axis=-1, keepdims=True)
        context = jnp.dot(new.astype(BF16), fresh[q, :, :LAT], preferred_element_type=F32)
        for j in range(KEY_BLOCKS):
            prob = jnp.exp2((old[j] - peak) * score_scale)
            weight = weight + jnp.sum(prob, axis=-1, keepdims=True)
            context = context + lax.dot_general(
                prob.astype(BF16),
                keys[q, :LAT, j * key_w : (j + 1) * key_w],
                across,
                preferred_element_type=F32,
            )
        ctx32[q] = context * (1.0 / weight)
        for j in range(n):
            first = (j * value_cols) // VH
            rows = [
                ctx32[q, t * heads + first : t * heads + first + heads_per, :]
                for t in range(steps)
            ]
            ctx_ref[q, j] = jnp.concatenate(rows, axis=0).astype(BF16)

    def ctx_start(q):
        def one(to):
            send(
                ctx_ref.at[q, to],
                ctx_in.at[q, my_slot],
                ctx_send.at[0],
                ctx_recv.at[q],
                to,
            ).start()

        for aa in far_first:
            loop(fan, lambda i: one(aa * fan + (me + i) % fan))
        loop(fan, lambda i: one(a * fan + (me + i) % fan), 1)

    with jax.named_scope('new_wait'):
        new_copy.wait()
    for q in range(seqs):
        fresh[q, :steps, :] = new_ref[q]
    with jax.named_scope("attn0"):
        attend(0)
    with jax.named_scope("barrier"):
        pl.semaphore_wait(barrier, n - 1)
    with jax.named_scope("send0"):
        ctx_start(0)
    for q in range(1, seqs):
        with jax.named_scope("attn1"):
            attend(q)
        with jax.named_scope("send1"):
            ctx_start(q)

    with jax.named_scope("prep"):
        share_out[...] = jnp.zeros_like(share_out)
        ids_copy.wait()
        slots_copy.wait()
        lane = lax.broadcasted_iota(jnp.int32, (toks, EXPERTS), 1)
        named = jnp.zeros((toks, EXPERTS), F32)
        kept = jnp.zeros((toks, EXPERTS), F32)
        for k in range(TOP):
            hit = jnp.where(ids_ref[:, k : k + 1] == lane, 1.0, 0.0)
            named = named + hit
            kept = kept + jnp.where(slots_ref[:, k : k + 1] < CAP, hit, 0.0)
        resid_copy.wait()
        gain_copy.wait()
        per = part_w // LANES
        for ch in range(CHUNKS):
            rows = [resid[q, :, ch * part_w : (ch + 1) * part_w].astype(F32) for q in range(seqs)]
            hid[ch] = jnp.concatenate(rows, axis=0)
            wide = gain_in[ch * per : (ch + 1) * per, :].astype(F32)
            gain[ch] = jnp.concatenate([wide[k : k + 1] for k in range(per)], axis=1)
        vu_copy.wait()

    def fold_values(q):
        settle(ctx_in.at[q, pl.ds(0, n - 1)], ctx_recv.at[q])
        bunch = 8 // piece

        def put(g):
            tile = [ctx_in[q, g * bunch + h].astype(F32) for h in range(bunch)]
            rows32[pl.ds(pl.multiple_of(g * 8, 8), 8), :] = (
                jnp.concatenate(tile, axis=0) if bunch > 1 else tile[0]
            )

        loop(n // bunch, put)
        mixed = jnp.dot(rows32[...].astype(BF16), vu[...], preferred_element_type=F32)
        shape = (n * piece, value_cols)
        row_head = lax.broadcasted_iota(jnp.int32, shape, 0) % heads_per
        col_head = lax.broadcasted_iota(jnp.int32, shape, 1) // (value_cols // heads_per)
        mixed = jnp.where(row_head == col_head, mixed, 0.0).astype(BF16)
        shape = (total, n * piece)
        came = lax.broadcasted_iota(jnp.int32, shape, 1)
        row_tok = (came // piece) * toks + q * steps + (came % piece) // heads_per
        fold = jnp.where(row_tok == lax.broadcasted_iota(jnp.int32, shape, 0), 1.0, 0.0)
        return jnp.dot(fold.astype(BF16), mixed, preferred_element_type=F32)

    for q in range(seqs):
        ctx_in[q, my_slot] = ctx_ref[q, me]
    folded = None
    for q in range(seqs):
        with jax.named_scope("values"):
            term = fold_values(q)
            folded = term if folded is None else folded + term
    values[...] = folded.astype(BF16)

    def reduce_scatter(product, finish):

        def core_copy(ch):
            return send(
                part.at[ch, 1 - c],
                in_core.at[ch],
                core_send.at[0],
                core_recv.at[0, ch],
                dev(a, b, 1 - c),
            )

        def mid_copy(ch, bb):
            return send(
                pair_sum.at[ch, bb],
                in_mid.at[ch, b],
                mid_send.at[0],
                mid_recv.at[0, ch],
                dev(a, bb, c),
            )

        def line_copy(ch, aa):
            return send(
                line_sum.at[ch, aa],
                in_line.at[ch, a],
                line_send.at[0],
                line_recv.at[0, ch],
                dev(aa, b, c),
            )

        def stage1(ch):
            whole = product(ch).astype(BF16).reshape(CORES, mids, group, part_w)
            part[ch] = whole
            core_copy(ch).start()

        def stage2(ch):
            settle(in_core.at[ch], core_recv.at[0, ch])

            def pair(bb):
                pair_sum[ch, bb] = (
                    part[ch, c, bb].astype(F32) + in_core[ch, bb].astype(F32)
                ).astype(BF16)

            def pair_send(i):
                bb = (b + i) % mids
                pair(bb)
                mid_copy(ch, bb).start()

            loop(mids, pair_send, 1)
            pair(b)

        def stage3(ch):
            settle(in_mid.at[ch, pl.ds(0, mids - 1)], mid_recv.at[0, ch])
            acc = pair_sum[ch, b].astype(F32)
            acc = lax.fori_loop(
                1, mids, lambda i, t: t + in_mid[ch, (b + i) % mids].astype(F32), acc
            )
            for aa in range(LINE):
                line_sum[ch, aa] = acc[aa * toks : (aa + 1) * toks].astype(BF16)
            for aa in far_first:
                line_copy(ch, aa).start()

        def stage4(ch):
            settle(in_line.at[ch, pl.ds(0, LINE - 1)], line_recv.at[0, ch])
            acc = line_sum[ch, a].astype(F32)
            for aa in far_first:
                acc = acc + in_line[ch, aa].astype(F32)
            finish(ch, acc)

        def drain():
            settle(in_core, core_send.at[0])
            settle(in_mid.at[:, pl.ds(0, mids - 1)], mid_send.at[0])
            settle(in_line.at[:, pl.ds(0, LINE - 1)], line_send.at[0])

        return (stage1, stage2, stage3, stage4), drain

    def attended_part(ch):
        if ch == 0:
            settle(op, w_sem.at[0])
        return jnp.dot(values[...], op[:, cols(ch)], preferred_element_type=F32)

    def spread_hidden(ch, acc):
        hidden = hid[ch] + acc
        hid[ch] = hidden
        block[ch, a] = (hidden * gain[ch]).astype(BF16)
        for aa in far_first:
            send(
                block.at[ch, a],
                block.at[ch, a],
                line_send.at[1],
                line_recv.at[1, ch],
                dev(aa, b, c),
            ).start()

    def hop_mid(ch):
        settle(block.at[ch, pl.ds(0, LINE - 1)], line_recv.at[1, ch])
        rows = [block[ch, aa].astype(F32) for aa in range(LINE)]
        gathered[ch, c, b] = jnp.concatenate(rows, axis=0).astype(BF16)
        ours = gathered.at[ch, c, b]

        def forward(i):
            send(
                ours, ours, mid_send.at[1], mid_recv.at[1, ch], dev(a, (b + i) % mids, c)
            ).start()

        loop(mids, forward, 1)

    def hop_core(ch):
        settle(gathered.at[ch, c, pl.ds(0, mids - 1)], mid_recv.at[1, ch])
        ours = gathered.at[ch, c]
        send(ours, ours, core_send.at[1], core_recv.at[1, ch], dev(a, b, 1 - c)).start()

    def multiply(ch):
        settle(gathered.at[ch, 1 - c], core_recv.at[1, ch])
        rows = gathered[ch].reshape(total, part_w)
        if ch == 0:
            settle(w_gate, w_sem.at[1])
            settle(w_up, w_sem.at[2])
        product = jnp.dot(rows, wgu[cols(ch), :], preferred_element_type=F32)
        if ch > 0:
            product = product + ffn_acc[...]
        ffn_acc[...] = product

    def route():
        router_copy.wait()
        square = jnp.zeros((toks, part_w), F32)
        logits = jnp.zeros((toks, EXPERTS), F32)
        for ch in range(CHUNKS):
            hidden = hid[ch]
            square = square + hidden * hidden
            logits = logits + lax.dot_general(
                block[ch, a],
                router[:, ch * part_w : (ch + 1) * part_w],
                across,
                preferred_element_type=F32,
            )
        scale = lax.rsqrt(jnp.sum(square, axis=-1, keepdims=True) / width + norm_eps)
        gates = jax.nn.sigmoid(logits * scale)
        shares = route_scale * gates / jnp.sum(gates * named, axis=1, keepdims=True) * kept
        share_out[:, :EXPERTS] = shares
        share_out[:, EXPERTS : EXPERTS + 1] = scale

        def share_start(i):
            send(
                share_out, share_in.at[my_slot], share_sem.at[0], share_sem.at[1], (me + i) % n
            ).start()

        loop(n, share_start, 1)
        share_in[my_slot] = share_out[...]

    first_stages, first_drain = reduce_scatter(attended_part, spread_hidden)

    def scoped(f):
        def g(*args):
            with jax.named_scope(f.__name__):
                f(*args)

        return g

    def run(stages, order, after=None):
        for stage, ch in order:
            scoped(stages[stage])(ch)
            if after is not None:
                after(stage, ch)

    def after_last(stage, ch):
        if (stage, ch) == (3, CHUNKS - 1):
            scoped(route)()

    with jax.named_scope("merged"):
        run(first_stages + (hop_mid, hop_core, multiply), MERGED, after_last)

    with jax.named_scope("act"):
        settle(share_in.at[pl.ds(0, n - 1)], share_sem.at[1])
        bunch = 8 // toks

        def put_share(g):
            tile = [share_in[g * bunch + h] for h in range(bunch)]
            share_all[pl.ds(pl.multiple_of(g * 8, 8), 8), :] = (
                jnp.concatenate(tile, axis=0) if bunch > 1 else tile[0]
            )

        loop(n // bunch, put_share)
        sent = share_all[...]
        mine = lax.broadcasted_iota(jnp.int32, share_all.shape, 1) == me // (n // EXPERTS)
        share = jnp.sum(jnp.where(mine, sent, 0.0), axis=1, keepdims=True)
        scale = sent[:, EXPERTS : EXPERTS + 1]
        gate = ffn_acc[:, :hidden_units] * scale
        up = ffn_acc[:, hidden_units:] * (scale * share)
        act[...] = (gate * jax.nn.sigmoid(gate) * up).astype(BF16)
        first_drain()

    def expert_part(ch):
        if ch == 0:
            settle(wd, w_sem.at[3])
        return jnp.dot(act[...], wd[:, cols(ch)], preferred_element_type=F32)

    def put_out(ch, acc):
        mixed = hid[ch] + acc
        for q in range(seqs):
            out_ref[q, :, cols(ch)] = mixed[q * steps : (q + 1) * steps].astype(BF16)
        pltpu.make_async_copy(out_ref.at[:, :, cols(ch)], out_hbm.at[:, :, cols(ch)], out_sem.at[0]).start()

    second_stages, second_drain = reduce_scatter(expert_part, put_out)
    with jax.named_scope("rs2"):
        run(second_stages, SECOND)

    with jax.named_scope("drain"):
        second_drain()
        settle(ctx_in.at[:, pl.ds(0, n - 1)], ctx_send.at[0])
        settle(share_in.at[pl.ds(0, n - 1)], share_sem.at[0])
        settle(block.at[:, pl.ds(0, LINE - 1)], line_send.at[1])
        settle(gathered.at[:, 0, pl.ds(0, mids - 1)], mid_send.at[1])
        settle(gathered.at[:, 0], core_send.at[1])
        pltpu.make_async_copy(out_ref, out_hbm, out_sem.at[0]).wait()


def body(
    cache_kv,
    new_kv,
    queries,
    lengths,
    resid,
    value_up,
    out_proj,
    norm_gain,
    router,
    expert_ids,
    slots,
    w_gate,
    w_up,
    w_down,
):
    n = lax.axis_size("ep")
    seqs, steps, heads, kv = queries.shape
    toks = seqs * steps
    width = resid.shape[-1]
    heads_per = max(1, value_up.shape[1] // VH)
    packets = (seqs, n, steps * heads_per, LAT)
    hidden_units = w_gate.shape[1]
    mids = n // (CORES * LINE)
    part_w = width // CHUNKS
    total = n * toks
    group = LINE * toks
    vmem = pl.BlockSpec(memory_space=pltpu.VMEM)
    hbm = pl.BlockSpec(memory_space=pl.ANY)
    landing = [
        pltpu.VMEM((CHUNKS, mids, group, part_w), BF16),
        pltpu.VMEM((CHUNKS, mids, group, part_w), BF16),
        pltpu.VMEM((CHUNKS, LINE, toks, part_w), BF16),
    ]
    dma = pltpu.SemaphoreType.DMA
    mixed = pl.pallas_call(
        functools.partial(layer_kernel, n),
        out_shape=jax.ShapeDtypeStruct(resid.shape, BF16),
        in_specs=[pl.BlockSpec(memory_space=pltpu.SMEM)] + [hbm] * 13,
        out_specs=hbm,
        scratch_shapes=[
            pltpu.VMEM(value_up.shape, BF16),
            pltpu.VMEM(out_proj.shape, BF16),
            pltpu.VMEM((width, 2 * hidden_units), BF16),
            pltpu.VMEM(w_down.shape, BF16),
            pltpu.VMEM((seqs, kv, cache_kv.shape[1]), BF16),
            pltpu.VMEM((seqs, LANES, kv), BF16),
            pltpu.VMEM((seqs, steps * heads, kv), BF16),
            pltpu.VMEM(new_kv.shape, BF16),
            pltpu.VMEM((width // LANES, LANES), BF16),
            pltpu.VMEM((CHUNKS, 1, part_w), F32),
            pltpu.VMEM((router.shape[1], width), BF16),
            pltpu.VMEM((toks, TOP), jnp.int32),
            pltpu.VMEM((toks, TOP), jnp.int32),
            pltpu.VMEM(resid.shape, BF16),
            pltpu.VMEM((seqs, steps * heads, LAT), F32),
            pltpu.VMEM(packets, BF16),
            pltpu.VMEM(packets, BF16),
            pltpu.VMEM((n * steps * heads_per, LAT), F32),
            pltpu.VMEM((total, value_up.shape[1]), BF16),
            pltpu.VMEM((total, hidden_units), BF16),
            pltpu.VMEM((total, 2 * hidden_units), F32),
            pltpu.VMEM((CHUNKS, toks, part_w), F32),
            pltpu.VMEM((CHUNKS, CORES, mids, group, part_w), BF16),
            pltpu.VMEM((CHUNKS, mids, group, part_w), BF16),
            pltpu.VMEM((CHUNKS, LINE, toks, part_w), BF16),
            *landing,
            pltpu.VMEM((CHUNKS, LINE, toks, part_w), BF16),
            pltpu.VMEM((CHUNKS, CORES, mids, group, part_w), BF16),
            pltpu.VMEM((toks, LANES), F32),
            pltpu.VMEM((n, toks, LANES), F32),
            pltpu.VMEM((total, LANES), F32),
            pltpu.VMEM(resid.shape, BF16),
            dma((1,)),
            dma((4,)),
            dma((7,)),
            dma((seqs, KEY_BLOCKS + 1)),
            dma((1,)),
            dma((seqs,)),
            dma((2,)),
            dma((2,)),
            dma((2, CHUNKS)),
            dma((2,)),
            dma((2, CHUNKS)),
            dma((2,)),
            dma((2, CHUNKS)),
        ],
        compiler_params=pltpu.CompilerParams(
            collective_id=0, has_side_effects=True, vmem_limit_bytes=67043328
        ),
    )(
        lengths,
        new_kv,
        norm_gain.reshape(width // LANES, LANES),
        router.T,
        expert_ids.reshape(toks, TOP),
        slots.reshape(toks, TOP),
        cache_kv.transpose(0, 2, 1),
        queries.reshape(seqs, steps * heads, kv),
        resid,
        value_up,
        out_proj,
        w_gate,
        w_up,
        w_down,
    )
    return mixed


def solution(mesh):
    return jax.shard_map(
        body,
        mesh=mesh,
        in_specs=(
            P(("rep", "ep"), None, None),
            P(("rep", "ep"), None, None),
            P(("rep", "ep"), None, None, None),
            P(("rep", "ep")),
            P(("rep", "ep"), None, None),
            P(None, "ep"),
            P("ep", None),
            P(),
            P(),
            P(("rep", "ep"), None, None),
            P(("rep", "ep"), None, None),
            P(None, "ep"),
            P(None, "ep"),
            P("ep", None),
        ),
        out_specs=P(("rep", "ep"), None, None),
        check_vma=False,
    )
```
